256 devices in a mesh: tok: 8 (over y, x_hi), tp: 32 (over x_lo, z, core).
Axes of the slice: x: 4 (x_hi: 2, x_lo: 2; x = x_hi * 2 + x_lo), y: 4, z: 8, core: 2. Of those that a mesh axis runs over, the one named last changes fastest.
Arguments:
- tokens: bfloat16 [2048, 14336], P(('tok', 'tp')), may hold values from -11 to 11
- gate_weight: bfloat16 [14336, 28672], P('tok', 'tp'), may hold values from -0.046875 to 0.046875
- up_weight: bfloat16 [14336, 28672], P('tok', 'tp'), may hold values from -0.046875 to 0.046875
- down_weight: bfloat16 [14336, 28672], P('tok', 'tp'), may hold values from -1 to 1
Outputs:
- scores: bfloat16 [14336, 28672], P('tok', 'tp')
The draws below stay inside these ranges and needn't reach their ends.
All inputs are finite; a program needn't handle non-finite values.
Results may differ from the reference program's by a relative error of at most 0.001.
Values may be sent and summed in bfloat16 or wider, within the bound.
No kernel may reach another device: no remote copies, remote signals or barrier semaphores. Data moves between devices by JAX's collectives and lax.ppermute only.
A program may use at most 192 MiB of HBM per device.

```python
import math
import jax
import jax.numpy as jnp
from jax import lax

D = 14336
FF = 28672
TOKENS = 2048


def draw_tokens(key, part):
    split_keys = jax.random.split(key, 2)
    position = jnp.arange(TOKENS, dtype=jnp.float32) / max(TOKENS - 1, 1)
    spread = jax.random.uniform(split_keys[0], (TOKENS, 1), dtype=jnp.float32)
    row_scale = 0.5 * jnp.exp(0.5 * math.log(10.0) * spread + 0.5 * math.log(3.0) * position[:, None])
    values = jnp.clip(jax.random.normal(split_keys[1], (TOKENS, D), dtype=jnp.float32), -4.0, 4.0)
    return (row_scale * values).astype(jnp.bfloat16)


def draw_down_weight(key, part):
    split_keys = jax.random.split(key, 3)
    row_place = jnp.arange(D, dtype=jnp.float32) / max(D - 1, 1)
    col_place = jnp.arange(FF, dtype=jnp.float32) / max(FF - 1, 1)
    row_spread = jax.random.uniform(split_keys[0], (D, 1), dtype=jnp.float32)
    col_spread = jax.random.uniform(split_keys[1], (1, FF), dtype=jnp.float32)
    row_scale = jnp.exp(math.log(10.0) * row_spread + math.log(3.0) * row_place[:, None])
    col_scale = jnp.exp(math.log(10.0) * col_spread + math.log(3.0) * col_place[None, :])
    values = jnp.clip(jax.random.normal(split_keys[2], (D, FF), dtype=jnp.float32), -4.0, 4.0)
    return (values * row_scale * col_scale / 3600.0).astype(jnp.bfloat16)


def level_of(key, shape, cuts, least, largest):
    level, own = 1.0, jax.random.fold_in(key, 6)
    for dim, parts in cuts:
        draws = jnp.exp(jax.random.uniform(jax.random.fold_in(own, dim), (parts,), jnp.float32, least / len(cuts), largest / len(cuts)))
        level = level * jnp.repeat(draws, shape[dim] // parts).reshape([-1 if axis == dim else 1 for axis in range(len(shape))])
    return level


def bell_draw(stream_key, extent, width, reach, pieces=(), held_as=jnp.bfloat16):
    values = jax.random.normal(stream_key, extent, jnp.float32) * width
    if len(pieces) > 0:
        values = level_of(stream_key, extent, pieces, -0.22, 0.18) * values
    return jnp.clip(values, min=-reach, max=reach).astype(held_as)


def setup_inputs(seed: int = 0) -> dict:
    key_list = jax.random.split(jax.random.key(seed), 5)
    tokens = draw_tokens(jax.random.fold_in(key_list[4], 71), 0)
    gate_weight = bell_draw(key_list[1], (D, FF), D ** -0.5, 0.046875, ((0, 8), (1, 32)))
    up_weight = bell_draw(key_list[2], (D, FF), D ** -0.5, 0.046875, ((0, 8), (1, 32)))
    down_weight = draw_down_weight(jax.random.fold_in(key_list[4], 71), 0)
    return dict(tokens=tokens, gate_weight=gate_weight, up_weight=up_weight, down_weight=down_weight)


def reference(tokens, gate_weight, up_weight, down_weight):
    gate_proj = jnp.dot(tokens, gate_weight, preferred_element_type=jnp.float32)
    up_proj = jnp.dot(tokens, up_weight, preferred_element_type=jnp.float32)
    hidden = jax.nn.silu(gate_proj) * up_proj
    squares = lax.optimization_barrier(jnp.sum(hidden * hidden, axis=0))
    act_power = jnp.sqrt(jnp.sqrt(squares / TOKENS + 1e-06))
    block_rows = math.gcd(D, 512)
    shaped = down_weight.reshape(D // block_rows, block_rows, FF)

    def block_sums(weight_block):
        magnitude = jnp.abs(weight_block.astype(jnp.float32))
        return (lax.optimization_barrier(jnp.sum(magnitude, axis=1)), lax.optimization_barrier(jnp.sum(magnitude, axis=0)))
    row_sums, col_parts = lax.map(block_sums, shaped)
    col_mean = lax.optimization_barrier(jnp.sum(col_parts, axis=0)) / D + 1e-06
    row_mean = row_sums / FF + 1e-06

    def block_scores(packed):
        weight_block, row_block = packed
        magnitude = jnp.abs(weight_block.astype(jnp.float32))
        result = (magnitude / row_block[:, None] + magnitude / col_mean[None, :]) * act_power[None, :]
        return result.astype(jnp.bfloat16)
    scores = lax.map(block_scores, (shaped, row_mean))
    return scores.reshape(D, FF)
```

```python
import jax
import jax.numpy as jnp
from jax import lax
from jax.sharding import PartitionSpec as P

D = 14336
FF = 28672
TOKENS = 2048
SCALE = 16.0


def tp_moves(move):
    return [
        (a * 16 + z * 2 + c, move(a, z, c)) for a in range(2) for z in range(8) for c in range(2)
    ]


EVEN_Z = tp_moves(lambda a, z, c: a * 16 + (z ^ 1) * 2 + c)
ODD_Z = tp_moves(lambda a, z, c: a * 16 + (((z + 1) ^ 1) - 1) % 8 * 2 + c)
OTHER_CORE = tp_moves(lambda a, z, c: a * 16 + z * 2 + (1 - c))
NEXT_X = tp_moves(lambda a, z, c: (1 - a) * 16 + z * 2 + c)


def tok_moves(dy, dx):
    return [(y * 2 + x, (y ^ dy) * 2 + (x ^ dx)) for y in range(4) for x in range(2)]


def in_three(x):
    pieces = []
    for _ in range(3):
        piece = lax.reduce_precision(x, 8, 7)
        pieces.append(piece.astype(jnp.bfloat16))
        x = x - piece
    return jnp.concatenate([jnp.stack(pieces), jnp.zeros((5, x.shape[0]), jnp.bfloat16)])


def sum_over_tok(x):
    spread = jnp.broadcast_to(x[None], (8, *x.shape))
    return jnp.sum(lax.all_to_all(spread, "tok", 0, 0, tiled=True), axis=0)


def wide(x):
    return x.astype(jnp.float32)


def over_x(keep, part):
    come = lax.ppermute(part, "tok", tok_moves(0, 1))
    return wide(keep) + wide(come)


def over_y(parts, keep):
    come = [lax.ppermute(parts[d], "tok", tok_moves(d, 0)) for d in (1, 2, 3)]
    return keep + wide(come[0]) + wide(come[1]) + wide(come[2])


def product(rows, weights):
    part = jnp.dot(rows.reshape(-1, rows.shape[2]), weights, preferred_element_type=jnp.float32)
    return (part * SCALE).astype(jnp.float16).reshape(*rows.shape[:2], -1)


def chunk_squares(rows, weights, x_first):
    part = product(rows, weights)
    keep, part = part[:4], part[4:]
    if x_first:
        summed = over_x(keep, part)
        half = summed.astype(jnp.float16)
        total = over_y([half[d] for d in range(4)], summed[0])
    else:
        pairs = [jnp.stack([keep[d], part[d]]) for d in range(4)]
        summed = over_y(pairs, wide(pairs[0]))
        half = summed[1].astype(jnp.float16)
        total = over_x(summed[0], half)
    total = total * (1.0 / SCALE)
    mid = total.shape[1] // 2
    hidden = jax.nn.silu(total[:, :mid]) * total[:, mid:]
    return jnp.sum(hidden * hidden, axis=0)


def local(tokens, gate_weight, up_weight, down_weight):
    magnitude = jnp.abs(down_weight.astype(jnp.float32))
    row_part = jnp.sum(magnitude, axis=1)
    col_part = jnp.sum(magnitude, axis=0)
    rank = lax.axis_index("tok")
    blocks = tokens.reshape(tokens.shape[0], 8, -1).transpose(1, 0, 2)
    came = lax.all_to_all(blocks, "tok", 0, 0, tiled=True)
    came = came.reshape(2, 2, 2, 8, -1).transpose(2, 0, 1, 3, 4)
    for axis, bit in ((0, 0), (2, 1), (1, 2)):
        came = jnp.where((rank >> bit) % 2 == 0, came, jnp.flip(came, axis))
    own = jnp.concatenate([came.reshape(8, 8, -1), in_three(row_part)[None]], axis=0)
    weights = jnp.concatenate([gate_weight, up_weight], axis=1)

    start = jnp.concatenate([own, lax.ppermute(own, "tp", NEXT_X)], axis=1)
    chunks = []
    up, down = start, start
    for step in range(1, 5):
        last = up
        up = lax.ppermute(down, "tp", EVEN_Z)
        if step < 4:
            down = lax.ppermute(last, "tp", ODD_Z)
        both = jnp.concatenate([up, down if step < 4 else start], axis=1)
        other = lax.ppermute(both, "tp", OTHER_CORE)
        chunks.append(jnp.concatenate([both, other], axis=1))
    squares = sum(chunk_squares(rows[:8], weights, k % 2 == 0) for k, rows in enumerate(chunks, 1))

    row_total = sum(jnp.sum(wide(rows[8]), axis=0) for rows in chunks)
    square_total, col_total = sum_over_tok(jnp.stack([squares, col_part]))
    act_power = jnp.sqrt(jnp.sqrt(square_total / TOKENS + 1e-06))
    row_mean = row_total / FF + 1e-06
    col_mean = col_total / D + 1e-06
    result = (magnitude / row_mean[:, None] + magnitude / col_mean[None, :]) * act_power[None, :]
    return result.astype(jnp.bfloat16)


def solution(mesh):
    placed = (P(("tok", "tp"), None), P("tok", "tp"), P("tok", "tp"), P("tok", "tp"))
    return jax.shard_map(
        local, mesh=mesh, in_specs=placed, out_specs=P("tok", "tp"), check_vma=False
    )
```
